32 devices in a mesh: grp: 2 (over y), col: 4 (over z), slc: 2 (over x), bat: 2 (over core).
Axes of the slice: x: 2, y: 2, z: 4, core: 2. Of those that a mesh axis runs over, the one named last changes fastest.
Arguments:
- site_tensors: bfloat16 [4, 72, 2, 64, 128], P(('grp', 'slc'), 'col'), parts along dimension 0, may hold values from -1.2 to 1.2
- left_edge: float32 [4, 64, 128], P(('grp', 'slc')), parts along dimension 0, may hold values from -0.5 to 0.5
- right_edge: float32 [4, 64, 128], P(('grp', 'slc')), parts along dimension 0, may hold values from -0.5 to 0.5
- order: int32 [144], P(('grp', 'col')), parts along dimension 0, may hold values from 0 to 71, each once
- bitstrings: int32 [128, 72], P(('grp', 'bat')), parts along dimension 0, may hold values 0 or 1
Outputs:
- amplitudes: float32 [2, 128], P(None, ('grp', 'bat')), parts along dimension 1
The draws below stay inside these ranges and needn't reach their ends.
There are 2 independent parts, one for each index of `grp`. The reference program is written for one: setup_inputs(seed, part) draws one part's arguments, and reference() takes and returns one part's arrays. A program takes and returns all parts, laid end to end along the dimension named above; each array names one. Nothing has to cross between parts.
Inputs may be any that keep to these rules, and one draw needn't show every extreme that they name: `order`: a permutation of the 72 qubit indices.
All inputs are finite; a program needn't handle non-finite values. No bound on the sum of `bitstrings` on one device may be relied on, other than what follows from the above.
Results may differ from the reference program's by a relative error of at most 0.0003.
Values sent between devices are 32-bit elements; how exact they have to be, the bound alone decides.
A program may use at most 64 MiB of HBM per device.

```python
import math
import jax
import jax.numpy as jnp
from jax import lax

CHI = 64
NQ = 72
BITS = 64
SLICES = 2


def batch_product(left_factor, right_factor):
    return jnp.einsum('nij,njk->nik', left_factor, right_factor, precision=lax.Precision.HIGHEST)


def complex_batch(left_real, left_imag, right_real, right_imag):
    real_part = batch_product(left_real, right_real) - batch_product(left_imag, right_imag)
    imag_part = batch_product(left_real, right_imag) + batch_product(left_imag, right_real)
    return (real_part, imag_part)


def draw_site_tensors(key, part):
    matrix_count = SLICES * NQ * 2
    subkeys = jax.random.split(jax.random.fold_in(key, 7103), 3)
    shape = (matrix_count, CHI, CHI)
    spread = math.sqrt(1.0 / (2.0 * CHI))
    noise_real = jax.random.normal(subkeys[0], shape, jnp.float32) * spread
    noise_imag = jax.random.normal(subkeys[1], shape, jnp.float32) * spread
    unit_matrix = jnp.eye(CHI, dtype=jnp.float32)
    current_real = (2.0 * unit_matrix[None] + noise_real) / 3.2
    current_imag = noise_imag / 3.2
    for sweep_index in range(10):
        adjoint_real = jnp.swapaxes(current_real, 1, 2)
        adjoint_imag = -jnp.swapaxes(current_imag, 1, 2)
        gram_real, gram_imag = complex_batch(adjoint_real, adjoint_imag, current_real, current_imag)
        cubic_real, cubic_imag = complex_batch(current_real, current_imag, gram_real, gram_imag)
        current_real = 1.5 * current_real - 0.5 * cubic_real
        current_imag = 1.5 * current_imag - 0.5 * cubic_imag
    matrix_gain = jnp.exp(jax.random.uniform(subkeys[2], (matrix_count, 1, 1), jnp.float32, -0.05, 0.05))
    current_real = current_real * matrix_gain
    current_imag = current_imag * matrix_gain
    joined = jnp.concatenate([current_real, current_imag], axis=-1)
    return joined.reshape(SLICES, NQ, 2, CHI, 2 * CHI).astype(jnp.bfloat16)


def plant(drawn, rng, smallest, high):
    dims = drawn.shape
    place = [jax.random.randint(jax.random.fold_in(rng, axis), (), 0, dims[axis]) for axis in range(len(dims))]
    drawn = drawn.at[tuple(place)].set(smallest)
    longest = dims.index(max(dims))
    place[longest] = (place[longest] + 1) % dims[longest]
    return drawn.at[tuple(place)].set(high)


def block_levels(key, shape, pieces, least, high):
    level, own = 1.0, jax.random.fold_in(key, 6)
    for axis_at, shards_of in pieces:
        draws = jnp.exp(jax.random.uniform(jax.random.fold_in(own, axis_at), (shards_of,), jnp.float32, least / len(pieces), high / len(pieces)))
        level = level * jnp.repeat(draws, shape[axis_at] // shards_of).reshape([-1 if axis == axis_at else 1 for axis in range(len(shape))])
    return level


def normal_values(stream_key, shape, deviation, most, cuts=(), kind=jnp.bfloat16):
    result = jax.random.normal(stream_key, shape, jnp.float32) * deviation
    if len(cuts) > 0:
        result = block_levels(stream_key, shape, cuts, -0.22, 0.18) * result
    return jnp.clip(result, min=-most, max=most).astype(kind)


def setup_inputs(seed: int = 0, part: int = 0) -> dict:
    key_of = jax.random.split(jax.random.key(seed), 6)
    part_keys = jax.random.split(jax.random.fold_in(key_of[5], part), 6)
    return {
        "site_tensors": draw_site_tensors(jax.random.fold_in(jax.random.fold_in(key_of[5], part), 71), part),
        "left_edge": normal_values(part_keys[1], (SLICES, CHI, 2 * CHI), (2 * CHI) ** -0.5, 0.5, ((0, 2),), jnp.float32),
        "right_edge": normal_values(part_keys[2], (SLICES, CHI, 2 * CHI), (2 * CHI) ** -0.5, 0.5, ((0, 2),), jnp.float32),
        "order": jax.random.permutation(part_keys[3], NQ).astype(jnp.int32),
        "bitstrings": plant((jax.random.randint(part_keys[4], (BITS, NQ), 0, 2) < 1).astype(jnp.int32), jax.random.fold_in(part_keys[4], 1), 0, 1),
    }


def rotate(block):
    middle = block.shape[-1] // 2
    return jnp.concatenate([-block[..., middle:], block[..., :middle]], axis=-1)


def complex_product(first_factor, second_factor):
    stacked = jnp.concatenate([second_factor, rotate(second_factor)], axis=-2)
    return jnp.einsum("bij,bjk->bik", first_factor, stacked, precision=lax.Precision.HIGHEST)


def closing(boundary, edge):
    real_left = boundary[..., :CHI]
    imag_left = boundary[..., CHI:]
    real_right = edge[..., :CHI]
    imag_right = edge[..., CHI:]
    real_part = jnp.sum(real_left * real_right - imag_left * imag_right, axis=(1, 2))
    imag_part = jnp.sum(real_left * imag_right + imag_left * real_right, axis=(1, 2))
    return jnp.stack([real_part, imag_part])


def slice_amplitude(operands, site_bits):
    tensors, left_start, right_stop = operands
    opening = jnp.broadcast_to(left_start, (BITS, CHI, 2 * CHI)).astype(jnp.float32)

    def advance(boundary, site_item):
        matrices, chosen_bits = site_item
        matrices = matrices.astype(jnp.float32)
        chosen = jnp.where(chosen_bits[:, None, None] == 1, matrices[1], matrices[0])
        return complex_product(boundary, chosen), None

    final_state, unused = lax.scan(advance, opening, (tensors, site_bits))
    return closing(final_state, right_stop)


def reference(site_tensors, left_edge, right_edge, order, bitstrings):
    site_bits = jnp.take(bitstrings, order.astype(jnp.int32), axis=1).T
    per_slice = lax.map(lambda operands: slice_amplitude(operands, site_bits), (site_tensors, left_edge, right_edge))
    return jnp.sum(per_slice, axis=0)
```

```python
import functools

import jax
import jax.numpy as jnp
from jax import lax
from jax.experimental import pallas as pl
from jax.experimental.pallas import tpu as pltpu
from jax.sharding import PartitionSpec as P

MESH = pl.DeviceIdType.MESH
GROUPS = 4
PIECES = 2
UNROLL = 2


def split(x):
    high = x.astype(jnp.bfloat16)
    low = (x - high.astype(jnp.float32)).astype(jnp.bfloat16)
    return high, low


def rotate(block):
    lanes = lax.broadcasted_iota(jnp.int32, block.shape, block.ndim - 1)
    middle = block.shape[-1] // 2
    rolled = pltpu.roll(block, middle, block.ndim - 1)
    return jnp.where(lanes < middle, -rolled, rolled)


def complex_product(first, second):
    first_high, first_low = split(first)
    high, low = split(second)
    turned_high, turned_low = split(rotate(second))
    left = jnp.concatenate([first_high, first_low], axis=0)
    right = jnp.concatenate(
        [
            jnp.concatenate([high, low], axis=1),
            jnp.concatenate([turned_high, turned_low], axis=1),
        ],
        axis=0,
    )
    out = jnp.dot(left, right, preferred_element_type=jnp.float32)
    chi = first.shape[0]
    wide = first.shape[1]
    small = out[:chi, wide:] + out[chi:, :wide] + out[chi:, wide:]
    return out[:chi, :wide] + small


def kernel(
    n_col,
    n_slc,
    groups,
    pieces,
    order_ref,
    bits_ref,
    tensors_ref,
    left_ref,
    right_ref,
    out_ref,
    weights,
    state,
    start,
    mine,
    arrived,
    closing_rows,
    share,
    finals,
    send_right,
    recv_right,
    send_left,
    recv_left,
    send_final,
    recv_final,
):
    col = lax.axis_index("col")
    slc = lax.axis_index("slc")
    sites = tensors_ref.shape[1]
    chi, wide = tensors_ref.shape[3], tensors_ref.shape[4]
    batch = bits_ref.shape[0]
    half = batch // 2
    per = half // groups
    chunk = per // pieces
    peers = n_col * n_slc
    me = col * n_slc + slc
    last = n_col - 1

    barrier = pltpu.get_barrier_semaphore()

    def greet(peer, carry):
        @pl.when(peer != me)
        def _():
            pl.semaphore_signal(
                barrier,
                inc=1,
                device_id={"col": peer // n_slc, "slc": lax.rem(peer, n_slc)},
                device_id_type=MESH,
            )

        return carry

    lax.fori_loop(0, peers, greet, 0)

    def build(site, carry):
        for bit in range(2):
            matrix = tensors_ref[0, site, bit].astype(jnp.float32)
            turned = rotate(matrix).astype(jnp.bfloat16)
            plain = matrix.astype(jnp.bfloat16)
            lanes = pl.ds(bit * wide, wide)
            for copy in range(2):
                weights[site, pl.ds(copy * wide, chi), lanes] = plain
                weights[site, pl.ds(copy * wide + chi, chi), lanes] = turned
        return carry

    lax.fori_loop(0, sites, build, 0)

    rows = lax.broadcasted_iota(jnp.int32, (chi, wide), 0)
    lanes = lax.broadcasted_iota(jnp.int32, (chi, wide), 1)
    unit = (rows == lanes).astype(jnp.float32)
    is_first = jnp.broadcast_to(col, (chi, wide)) == 0
    begin = jnp.where(is_first, left_ref[0], unit)
    begin_high, begin_low = split(begin)
    start[:, :wide] = begin_high
    start[:, wide:] = begin_low
    closing_rows[...] = jnp.zeros_like(closing_rows)

    def right_copy(piece):
        where = pl.ds(piece * chunk, chunk)
        return pltpu.make_async_remote_copy(
            src_ref=mine.at[where],
            dst_ref=arrived.at[where],
            send_sem=send_right.at[piece],
            recv_sem=recv_right.at[piece],
            device_id={"col": lax.rem(col + 1, n_col)},
            device_id_type=MESH,
        )

    def left_copy(piece):
        where = pl.ds(half + piece * chunk, chunk)
        return pltpu.make_async_remote_copy(
            src_ref=mine.at[where],
            dst_ref=arrived.at[where],
            send_sem=send_left.at[piece],
            recv_sem=recv_left.at[piece],
            device_id={"col": lax.rem(col + last, n_col)},
            device_id_type=MESH,
        )

    def item_of(group, at):
        base = 0 if at < per else half - per
        return base + group * per + at

    def advance(site, group, final):
        qubit = order_ref[site]
        block = weights[site]
        for at in range(2 * per):
            where = pl.ds(at * chi, chi)
            both = jnp.dot(state[where, :], block, preferred_element_type=jnp.float32)
            item = item_of(group, at)
            bit = jnp.broadcast_to(bits_ref[item, qubit], (chi, wide))
            chosen = jnp.where(bit == 1, both[:, wide:], both[:, :wide])
            if final:
                mine[item] = chosen
            else:
                high, low = split(chosen)
                state[where, :wide] = high
                state[where, wide:] = low

    def column(group):
        for at in range(2 * per):
            state[pl.ds(at * chi, chi), :] = start[...]

        def step(site, carry):
            advance(site, group, False)
            return carry

        lax.fori_loop(0, sites - 1, step, 0, unroll=UNROLL)
        advance(sites - 1, group, True)

    def close(item, row, value):
        edge = right_ref[0]
        turned = rotate(edge)
        signed = jnp.where(lanes < chi, edge, -edge)
        crossed = jnp.where(lanes < chi, -turned, turned)
        real_row = jnp.sum(value * signed, axis=0, keepdims=True)
        imag_row = jnp.sum(value * crossed, axis=0, keepdims=True)
        closing_rows[pl.ds(row, 1), :] = real_row
        closing_rows[pl.ds(half + row, 1), :] = imag_row

    def merge_right(group):
        for piece_at in range(pieces):
            piece = group * pieces + piece_at
            right_copy(piece).wait_recv()
            for at in range(chunk):
                item = piece * chunk + at
                mine[item] = complex_product(arrived[item], mine[item])

            @pl.when(col < last)
            def _():
                right_copy(piece).start()

            @pl.when(col == last)
            def _():
                for at in range(chunk):
                    item = piece * chunk + at
                    close(item, item, mine[item])

    def merge_left(group):
        for piece_at in range(pieces):
            piece = group * pieces + piece_at
            left_copy(piece).wait_recv()
            for at in range(chunk):
                item = half + piece * chunk + at
                mine[item] = complex_product(mine[item], arrived[item])

            @pl.when(col > 0)
            def _():
                left_copy(piece).start()

            @pl.when(col == 0)
            def _():
                for at in range(chunk):
                    item = half + piece * chunk + at
                    close(item, piece * chunk + at, mine[item])

    def slot(turn, carry):
        @pl.when(turn < groups)
        def _():
            column(turn)

            @pl.when(turn == 0)
            def _():
                pl.semaphore_wait(barrier, peers - 1)

            @pl.when(col == 0)
            def _():
                for at in range(pieces):
                    right_copy(turn * pieces + at).start()

            @pl.when(col == last)
            def _():
                for at in range(pieces):
                    left_copy(turn * pieces + at).start()

        from_left = turn - col

        @pl.when((col > 0) & (from_left >= 0) & (from_left < groups))
        def _():
            merge_right(from_left)

        from_right = turn - (last - col)

        @pl.when((col < last) & (from_right >= 0) & (from_right < groups))
        def _():
            merge_left(from_right)

        return carry

    lax.fori_loop(0, groups + last, slot, 0)

    def final_copy(peer, place):
        return pltpu.make_async_remote_copy(
            src_ref=share,
            dst_ref=finals.at[place],
            send_sem=send_final.at[peer],
            recv_sem=recv_final.at[place],
            device_id={"col": peer // n_slc, "slc": lax.rem(peer, n_slc)},
            device_id_type=MESH,
        )

    closer = (col == 0) | (col == last)
    place = jnp.where(col == last, slc, n_slc + slc)

    @pl.when(closer)
    def _():
        totals = jnp.sum(closing_rows[...].T, axis=0, keepdims=True)
        tile = jnp.broadcast_to(totals, share.shape)
        share[...] = tile
        finals[place] = tile

        def send(peer, carry):
            @pl.when(peer != me)
            def _():
                final_copy(peer, place).start()

            return carry

        lax.fori_loop(0, peers, send, 0)

    for side in range(2):
        for part in range(n_slc):
            source_col = last if side == 0 else 0

            @pl.when((col != source_col) | (slc != part))
            def _():
                final_copy(me, side * n_slc + part).wait_recv()

    sums = []
    for side in range(2):
        total = finals[side * n_slc]
        for part in range(1, n_slc):
            total = total + finals[side * n_slc + part]
        sums.append(total)
    ahead, behind = sums
    columns = lax.broadcasted_iota(jnp.int32, share.shape, 1)
    width = share.shape[1]
    real = jnp.where(columns < half, ahead, pltpu.roll(behind, half, 1))
    imag = jnp.where(columns < half, pltpu.roll(ahead, width - half, 1), behind)
    out_ref[0:1, :] = real[0:1, :batch]
    out_ref[1:2, :] = imag[0:1, :batch]

    @pl.when(closer)
    def _():
        def done(peer, carry):
            @pl.when(peer != me)
            def _():
                final_copy(peer, place).wait_send()

            return carry

        lax.fori_loop(0, peers, done, 0)

    @pl.when(col < last)
    def _():
        for piece in range(groups * pieces):
            right_copy(piece).wait_send()

    @pl.when(col > 0)
    def _():
        for piece in range(groups * pieces):
            left_copy(piece).wait_send()


def on_device(site_tensors, left_edge, right_edge, order, bitstrings):
    n_col = lax.axis_size("col")
    n_slc = lax.axis_size("slc")
    batch = bitstrings.shape[0]
    half = batch // 2
    groups = GROUPS
    pieces = PIECES
    sites, chi, wide = site_tensors.shape[1], site_tensors.shape[3], site_tensors.shape[4]
    peers = n_col * n_slc
    chunks = groups * pieces
    vmem = pl.BlockSpec(memory_space=pltpu.VMEM)
    smem = pl.BlockSpec(memory_space=pltpu.SMEM)
    lane_rows = 128
    return pl.pallas_call(
        functools.partial(kernel, n_col, n_slc, groups, pieces),
        out_shape=jax.ShapeDtypeStruct((2, batch), jnp.float32),
        in_specs=[smem, smem, vmem, vmem, vmem],
        out_specs=vmem,
        scratch_shapes=[
            pltpu.VMEM((sites, 2 * wide, 2 * wide), jnp.bfloat16),
            pltpu.VMEM((batch // groups * chi, 2 * wide), jnp.bfloat16),
            pltpu.VMEM((chi, 2 * wide), jnp.bfloat16),
            pltpu.VMEM((batch, chi, wide), jnp.float32),
            pltpu.VMEM((batch, chi, wide), jnp.float32),
            pltpu.VMEM((lane_rows, wide), jnp.float32),
            pltpu.VMEM((8, lane_rows), jnp.float32),
            pltpu.VMEM((2 * n_slc, 8, lane_rows), jnp.float32),
            pltpu.SemaphoreType.DMA((chunks,)),
            pltpu.SemaphoreType.DMA((chunks,)),
            pltpu.SemaphoreType.DMA((chunks,)),
            pltpu.SemaphoreType.DMA((chunks,)),
            pltpu.SemaphoreType.DMA((peers,)),
            pltpu.SemaphoreType.DMA((2 * n_slc,)),
        ],
        compiler_params=pltpu.CompilerParams(collective_id=0, has_side_effects=True),
    )(order, bitstrings, site_tensors, left_edge, right_edge)


def solution(mesh):
    return jax.shard_map(
        on_device,
        mesh=mesh,
        in_specs=(
            P(("grp", "slc"), "col", None, None, None),
            P(("grp", "slc"), None, None),
            P(("grp", "slc"), None, None),
            P(("grp", "col")),
            P(("grp", "bat"), None),
        ),
        out_specs=P(None, ("grp", "bat")),
        check_vma=False,
    )
```

```python
import functools

import jax
import jax.numpy as jnp
from jax import lax
from jax.experimental import pallas as pl
from jax.experimental.pallas import tpu as pltpu
from jax.sharding import PartitionSpec as P

MESH = pl.DeviceIdType.MESH
GROUPS = 8
PIECES = 1
LAG = 2
DEPTH = 5


def split(x):
    high = x.astype(jnp.bfloat16)
    low = (x - high.astype(jnp.float32)).astype(jnp.bfloat16)
    return high, low


def rotate(block):
    lanes = lax.broadcasted_iota(jnp.int32, block.shape, block.ndim - 1)
    middle = block.shape[-1] // 2
    rolled = pltpu.roll(block, middle, block.ndim - 1)
    return jnp.where(lanes < middle, -rolled, rolled)


def left_form(x):
    high, low = split(x)
    return jnp.concatenate([high, low], axis=0)


def right_form(x):
    high, low = split(x)
    turned_high, turned_low = split(rotate(x))
    return jnp.concatenate(
        [
            jnp.concatenate([high, low], axis=1),
            jnp.concatenate([turned_high, turned_low], axis=1),
        ],
        axis=0,
    )


def form_product(left, right):
    out = jnp.dot(left, right, preferred_element_type=jnp.float32)
    chi = left.shape[0] // 2
    wide = left.shape[1]
    small = out[:chi, wide:] + out[chi:, :wide] + out[chi:, wide:]
    return out[:chi, :wide] + small


def complex_product(first, second):
    return form_product(left_form(first), right_form(second))


def segments_of(sites):
    count = -(-sites // DEPTH)
    sizes = [sites // count + (1 if at < sites % count else 0) for at in range(count)]
    starts = [sum(sizes[:at]) for at in range(count)]
    return list(zip(starts, sizes))


def site_weights(first, second):
    plain = jnp.concatenate([first, second], axis=1)
    turned = jnp.concatenate(
        [
            rotate(first.astype(jnp.float32)).astype(jnp.bfloat16),
            rotate(second.astype(jnp.float32)).astype(jnp.bfloat16),
        ],
        axis=1,
    )
    return jnp.concatenate([plain, turned, plain, turned], axis=0)


def kernel(
    n_col,
    n_slc,
    groups,
    pieces,
    order_ref,
    bits_ref,
    tensors_ref,
    left_ref,
    right_ref,
    out_ref,
    state,
    first_table,
    other_table,
    mine,
    arrived,
    closing_rows,
    share,
    finals,
    send_right,
    recv_right,
    send_left,
    recv_left,
    send_final,
    recv_final,
):
    col = lax.axis_index("col")
    slc = lax.axis_index("slc")
    sites = tensors_ref.shape[1]
    chi, wide = tensors_ref.shape[3], tensors_ref.shape[4]
    batch = bits_ref.shape[0]
    half = batch // 2
    per = half // groups
    chunk = per // pieces
    peers = n_col * n_slc
    me = col * n_slc + slc
    last = n_col - 1

    barrier = pltpu.get_barrier_semaphore()

    def greet(peer, carry):
        @pl.when(peer != me)
        def _():
            pl.semaphore_signal(
                barrier,
                inc=1,
                device_id={"col": peer // n_slc, "slc": lax.rem(peer, n_slc)},
                device_id_type=MESH,
            )

        return carry

    lax.fori_loop(0, peers, greet, 0)

    rows = lax.broadcasted_iota(jnp.int32, (chi, wide), 0)
    lanes = lax.broadcasted_iota(jnp.int32, (chi, wide), 1)
    unit = (rows == lanes).astype(jnp.float32)
    is_first = jnp.broadcast_to(col, (chi, wide)) == 0
    begin = jnp.where(is_first, left_ref[0], unit)
    segments = segments_of(sites)
    bases = []
    entries = 0
    for at, (_, size) in enumerate(segments):
        bases.append(entries)
        entries += 0 if at == 0 else 2**size

    def put(segment, size, level, entry, value):
        if level < size:
            high, low = split(value)
            where = pl.ds(entry * chi, chi)
            state[segment, where, :wide] = high
            state[segment, where, wide:] = low
        elif segment == 0:
            first_table[entry] = left_form(value)
        else:
            other_table[bases[segment] + entry] = right_form(value)

    for level in range(DEPTH):
        for segment, (origin, size) in enumerate(segments):
            if level >= size:
                continue
            site = origin + level
            if level == 0 and segment > 0:
                for bit in range(2):
                    value = tensors_ref[0, site, bit].astype(jnp.float32)
                    put(segment, size, 1, bit, value)
                continue
            if level == 0:
                put(segment, size, 0, 0, begin)
            block = site_weights(tensors_ref[0, site, 0], tensors_ref[0, site, 1])
            for entry in range(2**level):
                source = state[segment, pl.ds(entry * chi, chi), :]
                both = jnp.dot(source, block, preferred_element_type=jnp.float32)
                put(segment, size, level + 1, entry, both[:, :wide])
                put(segment, size, level + 1, entry + 2**level, both[:, wide:])

    closing_rows[...] = jnp.zeros_like(closing_rows)

    def right_copy(piece):
        where = pl.ds(piece * chunk, chunk)
        return pltpu.make_async_remote_copy(
            src_ref=mine.at[where],
            dst_ref=arrived.at[where],
            send_sem=send_right.at[piece],
            recv_sem=recv_right.at[piece],
            device_id={"col": lax.rem(col + 1, n_col)},
            device_id_type=MESH,
        )

    def left_copy(piece):
        where = pl.ds(half + piece * chunk, chunk)
        return pltpu.make_async_remote_copy(
            src_ref=mine.at[where],
            dst_ref=arrived.at[where],
            send_sem=send_left.at[piece],
            recv_sem=recv_left.at[piece],
            device_id={"col": lax.rem(col + last, n_col)},
            device_id_type=MESH,
        )

    def item_of(group, at):
        base = 0 if at < per else half - per
        return base + group * per + at

    def column(group):
        for at in range(2 * per):
            item = item_of(group, at)
            value = None
            for segment, (origin, size) in enumerate(segments):
                entry = bits_ref[item, order_ref[origin]]
                for level in range(1, size):
                    bit = bits_ref[item, order_ref[origin + level]]
                    entry = entry + bit * 2**level
                if segment == 0:
                    left = first_table[entry]
                    continue
                right = other_table[bases[segment] + entry]
                value = form_product(left, right)
                if segment < len(segments) - 1:
                    left = left_form(value)
            mine[item] = value

    def close(item, row, value):
        edge = right_ref[0]
        turned = rotate(edge)
        signed = jnp.where(lanes < chi, edge, -edge)
        crossed = jnp.where(lanes < chi, -turned, turned)
        real_row = jnp.sum(value * signed, axis=0, keepdims=True)
        imag_row = jnp.sum(value * crossed, axis=0, keepdims=True)
        closing_rows[pl.ds(row, 1), :] = real_row
        closing_rows[pl.ds(half + row, 1), :] = imag_row

    def merge_right(group):
        for piece_at in range(pieces):
            piece = group * pieces + piece_at
            right_copy(piece).wait_recv()
            for at in range(chunk):
                item = piece * chunk + at
                mine[item] = complex_product(arrived[item], mine[item])

            @pl.when(col < last)
            def _():
                right_copy(piece).start()

            @pl.when(col == last)
            def _():
                for at in range(chunk):
                    item = piece * chunk + at
                    close(item, item, mine[item])

    def merge_left(group):
        for piece_at in range(pieces):
            piece = group * pieces + piece_at
            left_copy(piece).wait_recv()
            for at in range(chunk):
                item = half + piece * chunk + at
                mine[item] = complex_product(mine[item], arrived[item])

            @pl.when(col > 0)
            def _():
                left_copy(piece).start()

            @pl.when(col == 0)
            def _():
                for at in range(chunk):
                    item = half + piece * chunk + at
                    close(item, piece * chunk + at, mine[item])

    def slot(turn, carry):
        @pl.when(turn < groups)
        def _():
            column(turn)

            @pl.when(turn == 0)
            def _():
                pl.semaphore_wait(barrier, peers - 1)

            @pl.when(col == 0)
            def _():
                for at in range(pieces):
                    right_copy(turn * pieces + at).start()

            @pl.when(col == last)
            def _():
                for at in range(pieces):
                    left_copy(turn * pieces + at).start()

        from_left = turn - LAG * col

        @pl.when((col > 0) & (from_left >= 0) & (from_left < groups))
        def _():
            merge_right(from_left)

        from_right = turn - LAG * (last - col)

        @pl.when((col < last) & (from_right >= 0) & (from_right < groups))
        def _():
            merge_left(from_right)

        return carry

    lax.fori_loop(0, groups + LAG * last, slot, 0)

    def final_copy(peer, place):
        return pltpu.make_async_remote_copy(
            src_ref=share,
            dst_ref=finals.at[place],
            send_sem=send_final.at[peer],
            recv_sem=recv_final.at[place],
            device_id={"col": peer // n_slc, "slc": lax.rem(peer, n_slc)},
            device_id_type=MESH,
        )

    closer = (col == 0) | (col == last)
    place = jnp.where(col == last, slc, n_slc + slc)

    @pl.when(closer)
    def _():
        totals = jnp.sum(closing_rows[...].T, axis=0, keepdims=True)
        tile = jnp.broadcast_to(totals, share.shape)
        share[...] = tile
        finals[place] = tile

        def send(peer, carry):
            @pl.when(peer != me)
            def _():
                final_copy(peer, place).start()

            return carry

        lax.fori_loop(0, peers, send, 0)

    for side in range(2):
        for part in range(n_slc):
            source_col = last if side == 0 else 0

            @pl.when((col != source_col) | (slc != part))
            def _():
                final_copy(me, side * n_slc + part).wait_recv()

    sums = []
    for side in range(2):
        total = finals[side * n_slc]
        for part in range(1, n_slc):
            total = total + finals[side * n_slc + part]
        sums.append(total)
    ahead, behind = sums
    columns = lax.broadcasted_iota(jnp.int32, share.shape, 1)
    width = share.shape[1]
    real = jnp.where(columns < half, ahead, pltpu.roll(behind, half, 1))
    imag = jnp.where(columns < half, pltpu.roll(ahead, width - half, 1), behind)
    out_ref[0:1, :] = real[0:1, :batch]
    out_ref[1:2, :] = imag[0:1, :batch]

    @pl.when(closer)
    def _():
        def done(peer, carry):
            @pl.when(peer != me)
            def _():
                final_copy(peer, place).wait_send()

            return carry

        lax.fori_loop(0, peers, done, 0)

    @pl.when(col < last)
    def _():
        for piece in range(groups * pieces):
            right_copy(piece).wait_send()

    @pl.when(col > 0)
    def _():
        for piece in range(groups * pieces):
            left_copy(piece).wait_send()


def on_device(site_tensors, left_edge, right_edge, order, bitstrings):
    n_col = lax.axis_size("col")
    n_slc = lax.axis_size("slc")
    batch = bitstrings.shape[0]
    half = batch // 2
    groups = GROUPS
    pieces = PIECES
    sites, chi, wide = site_tensors.shape[1], site_tensors.shape[3], site_tensors.shape[4]
    peers = n_col * n_slc
    chunks = groups * pieces
    vmem = pl.BlockSpec(memory_space=pltpu.VMEM)
    smem = pl.BlockSpec(memory_space=pltpu.SMEM)
    lane_rows = 128
    sizes = [2**size for _, size in segments_of(sites)]
    return pl.pallas_call(
        functools.partial(kernel, n_col, n_slc, groups, pieces),
        out_shape=jax.ShapeDtypeStruct((2, batch), jnp.float32),
        in_specs=[smem, smem, vmem, vmem, vmem],
        out_specs=vmem,
        scratch_shapes=[
            pltpu.VMEM((len(sizes), max(sizes) // 2 * chi, 2 * wide), jnp.bfloat16),
            pltpu.VMEM((sizes[0], 2 * chi, wide), jnp.bfloat16),
            pltpu.VMEM((sum(sizes[1:]), 2 * chi, 2 * wide), jnp.bfloat16),
            pltpu.VMEM((batch, chi, wide), jnp.float32),
            pltpu.VMEM((batch, chi, wide), jnp.float32),
            pltpu.VMEM((lane_rows, wide), jnp.float32),
            pltpu.VMEM((8, lane_rows), jnp.float32),
            pltpu.VMEM((2 * n_slc, 8, lane_rows), jnp.float32),
            pltpu.SemaphoreType.DMA((chunks,)),
            pltpu.SemaphoreType.DMA((chunks,)),
            pltpu.SemaphoreType.DMA((chunks,)),
            pltpu.SemaphoreType.DMA((chunks,)),
            pltpu.SemaphoreType.DMA((peers,)),
            pltpu.SemaphoreType.DMA((2 * n_slc,)),
        ],
        compiler_params=pltpu.CompilerParams(collective_id=0, has_side_effects=True),
    )(order, bitstrings, site_tensors, left_edge, right_edge)


def solution(mesh):
    return jax.shard_map(
        on_device,
        mesh=mesh,
        in_specs=(
            P(("grp", "slc"), "col", None, None, None),
            P(("grp", "slc"), None, None),
            P(("grp", "slc"), None, None),
            P(("grp", "col")),
            P(("grp", "bat"), None),
        ),
        out_specs=P(None, ("grp", "bat")),
        check_vma=False,
    )
```

```python
import functools

import jax
import jax.numpy as jnp
from jax import lax
from jax.experimental import pallas as pl
from jax.experimental.pallas import tpu as pltpu
from jax.sharding import PartitionSpec as P

MESH = pl.DeviceIdType.MESH
GROUPS = 8
PIECES = 1
LAG = 3
DEPTH = 5


def split(x):
    high = x.astype(jnp.bfloat16)
    low = (x - high.astype(jnp.float32)).astype(jnp.bfloat16)
    return high, low


def rotate(block):
    lanes = lax.broadcasted_iota(jnp.int32, block.shape, block.ndim - 1)
    middle = block.shape[-1] // 2
    rolled = pltpu.roll(block, middle, block.ndim - 1)
    return jnp.where(lanes < middle, -rolled, rolled)


def left_form(x):
    high, low = split(x)
    return jnp.concatenate([high, low], axis=0)


def right_form(x):
    high, low = split(x)
    turned_high, turned_low = split(rotate(x))
    return jnp.concatenate(
        [
            jnp.concatenate([high, low], axis=1),
            jnp.concatenate([turned_high, turned_low], axis=1),
        ],
        axis=0,
    )


def form_product(left, right):
    out = jnp.dot(left, right, preferred_element_type=jnp.float32)
    chi = left.shape[0] // 2
    wide = left.shape[1]
    small = out[:chi, wide:] + out[chi:, :wide] + out[chi:, wide:]
    return out[:chi, :wide] + small


def complex_product(first, second):
    return form_product(left_form(first), right_form(second))


def segments_of(sites):
    count = -(-sites // DEPTH)
    sizes = [sites // count + (1 if at < sites % count else 0) for at in range(count)]
    starts = [sum(sizes[:at]) for at in range(count)]
    return list(zip(starts, sizes))


def site_weights(first, second):
    plain = jnp.concatenate([first, second], axis=1)
    turned = jnp.concatenate(
        [
            rotate(first.astype(jnp.float32)).astype(jnp.bfloat16),
            rotate(second.astype(jnp.float32)).astype(jnp.bfloat16),
        ],
        axis=1,
    )
    return jnp.concatenate([plain, turned, plain, turned], axis=0)


def kernel(
    n_col,
    n_slc,
    groups,
    pieces,
    order_ref,
    bits_ref,
    tensors_hbm,
    left_hbm,
    right_hbm,
    out_ref,
    tensors_ref,
    left_ref,
    right_ref,
    load_sem,
    state,
    first_table,
    other_table,
    mine,
    arrived,
    closing_rows,
    share,
    finals,
    send_right,
    recv_right,
    send_left,
    recv_left,
    send_final,
    recv_final,
):
    col = lax.axis_index("col")
    slc = lax.axis_index("slc")
    sites = tensors_ref.shape[1]
    chi, wide = tensors_ref.shape[3], tensors_ref.shape[4]
    batch = bits_ref.shape[0]
    half = batch // 2
    per = half // groups
    chunk = per // pieces
    peers = n_col * n_slc
    me = col * n_slc + slc
    last = n_col - 1

    barrier = pltpu.get_barrier_semaphore()

    def greet(where):
        pl.semaphore_signal(barrier, inc=1, device_id=where, device_id_type=MESH)

    @pl.when(col > 0)
    def _():
        greet({"col": lax.rem(col + last, n_col)})

    @pl.when(col < last)
    def _():
        greet({"col": lax.rem(col + 1, n_col)})

    for step in range(1, n_slc):
        greet({"slc": lax.rem(slc + step, n_slc)})

    loads = [
        pltpu.make_async_copy(tensors_hbm, tensors_ref, load_sem.at[0]),
        pltpu.make_async_copy(left_hbm, left_ref, load_sem.at[1]),
        pltpu.make_async_copy(right_hbm, right_ref, load_sem.at[2]),
    ]
    for load in loads:
        load.start()
    for load in loads:
        load.wait()

    rows = lax.broadcasted_iota(jnp.int32, (chi, wide), 0)
    lanes = lax.broadcasted_iota(jnp.int32, (chi, wide), 1)
    unit = (rows == lanes).astype(jnp.float32)
    is_first = jnp.broadcast_to(col, (chi, wide)) == 0
    begin = jnp.where(is_first, left_ref[0], unit)
    segments = segments_of(sites)
    bases = []
    entries = 0
    for at, (_, size) in enumerate(segments):
        bases.append(entries)
        entries += 0 if at == 0 else 2**size

    def put(segment, size, level, entry, value):
        if level < size:
            high, low = split(value)
            where = pl.ds(entry * chi, chi)
            state[segment, where, :wide] = high
            state[segment, where, wide:] = low
        elif segment == 0:
            first_table[entry] = left_form(value)
        else:
            other_table[bases[segment] + entry] = right_form(value)

    for level in range(DEPTH):
        for segment, (origin, size) in enumerate(segments):
            if level >= size:
                continue
            site = origin + level
            if level == 0 and segment > 0:
                for bit in range(2):
                    value = tensors_ref[0, site, bit].astype(jnp.float32)
                    put(segment, size, 1, bit, value)
                continue
            if level == 0:
                put(segment, size, 0, 0, begin)
            block = site_weights(tensors_ref[0, site, 0], tensors_ref[0, site, 1])
            for entry in range(2**level):
                source = state[segment, pl.ds(entry * chi, chi), :]
                both = jnp.dot(source, block, preferred_element_type=jnp.float32)
                put(segment, size, level + 1, entry, both[:, :wide])
                put(segment, size, level + 1, entry + 2**level, both[:, wide:])

    closing_rows[...] = jnp.zeros_like(closing_rows)

    def right_copy(piece):
        where = pl.ds(piece * chunk, chunk)
        return pltpu.make_async_remote_copy(
            src_ref=mine.at[where],
            dst_ref=arrived.at[where],
            send_sem=send_right.at[piece],
            recv_sem=recv_right.at[piece],
            device_id={"col": lax.rem(col + 1, n_col)},
            device_id_type=MESH,
        )

    def left_copy(piece):
        where = pl.ds(half + piece * chunk, chunk)
        return pltpu.make_async_remote_copy(
            src_ref=mine.at[where],
            dst_ref=arrived.at[where],
            send_sem=send_left.at[piece],
            recv_sem=recv_left.at[piece],
            device_id={"col": lax.rem(col + last, n_col)},
            device_id_type=MESH,
        )

    def item_of(group, at):
        base = 0 if at < per else half - per
        return base + group * per + at

    def column(group):
        items = [item_of(group, at) for at in range(2 * per)]
        values = []
        for segment, (origin, size) in enumerate(segments):
            qubits = [order_ref[origin + level] for level in range(size)]
            entries_of = []
            for item in items:
                entry = bits_ref[item, qubits[0]]
                for level in range(1, size):
                    entry = entry + bits_ref[item, qubits[level]] * 2**level
                entries_of.append(entry)
            if segment == 0:
                lefts = [first_table[entry] for entry in entries_of]
                continue
            if segment > 1:
                lefts = [left_form(value) for value in values]
            values = [
                form_product(left, other_table[bases[segment] + entry])
                for left, entry in zip(lefts, entries_of)
            ]
        for item, value in zip(items, values):
            mine[item] = value

    def close(item, row, value):
        edge = right_ref[0]
        turned = rotate(edge)
        signed = jnp.where(lanes < chi, edge, -edge)
        crossed = jnp.where(lanes < chi, -turned, turned)
        real_row = jnp.sum(value * signed, axis=0, keepdims=True)
        imag_row = jnp.sum(value * crossed, axis=0, keepdims=True)
        closing_rows[pl.ds(row, 1), :] = real_row
        closing_rows[pl.ds(half + row, 1), :] = imag_row

    def merge_right(group):
        for piece_at in range(pieces):
            piece = group * pieces + piece_at
            right_copy(piece).wait_recv()
            items = [piece * chunk + at for at in range(chunk)]
            values = [complex_product(arrived[item], mine[item]) for item in items]
            for item, value in zip(items, values):
                mine[item] = value

            @pl.when(col < last)
            def _():
                right_copy(piece).start()

            @pl.when(col == last)
            def _():
                for at in range(chunk):
                    item = piece * chunk + at
                    close(item, item, mine[item])

    def merge_left(group):
        for piece_at in range(pieces):
            piece = group * pieces + piece_at
            left_copy(piece).wait_recv()
            items = [half + piece * chunk + at for at in range(chunk)]
            values = [complex_product(mine[item], arrived[item]) for item in items]
            for item, value in zip(items, values):
                mine[item] = value

            @pl.when(col > 0)
            def _():
                left_copy(piece).start()

            @pl.when(col == 0)
            def _():
                for at in range(chunk):
                    item = half + piece * chunk + at
                    close(item, piece * chunk + at, mine[item])

    def slot(turn, carry):
        @pl.when(turn < groups)
        def _():
            column(turn)

            @pl.when(turn == 0)
            def _():
                near = jnp.where((col > 0) & (col < last), 2, 1)
                pl.semaphore_wait(barrier, near + n_slc - 1)

            @pl.when(col == 0)
            def _():
                for at in range(pieces):
                    right_copy(turn * pieces + at).start()

            @pl.when(col == last)
            def _():
                for at in range(pieces):
                    left_copy(turn * pieces + at).start()

        from_left = turn - LAG * col

        @pl.when((col > 0) & (from_left >= 0) & (from_left < groups))
        def _():
            merge_right(from_left)

        from_right = turn - LAG * (last - col)

        @pl.when((col < last) & (from_right >= 0) & (from_right < groups))
        def _():
            merge_left(from_right)

        return carry

    lax.fori_loop(0, groups + LAG * last, slot, 0)

    def final_copy(peer, place):
        return pltpu.make_async_remote_copy(
            src_ref=share,
            dst_ref=finals.at[place],
            send_sem=send_final.at[peer],
            recv_sem=recv_final.at[place],
            device_id={"col": peer // n_slc, "slc": lax.rem(peer, n_slc)},
            device_id_type=MESH,
        )

    closer = (col == 0) | (col == last)
    place = jnp.where(col == last, slc, n_slc + slc)

    @pl.when(closer)
    def _():
        totals = jnp.sum(closing_rows[...].T, axis=0, keepdims=True)
        tile = jnp.broadcast_to(totals, share.shape)
        share[...] = tile
        finals[place] = tile

        def send(peer, carry):
            @pl.when(peer != me)
            def _():
                final_copy(peer, place).start()

            return carry

        lax.fori_loop(0, peers, send, 0)

    for side in range(2):
        for part in range(n_slc):
            source_col = last if side == 0 else 0

            @pl.when((col != source_col) | (slc != part))
            def _():
                final_copy(me, side * n_slc + part).wait_recv()

    sums = []
    for side in range(2):
        total = finals[side * n_slc]
        for part in range(1, n_slc):
            total = total + finals[side * n_slc + part]
        sums.append(total)
    ahead, behind = sums
    columns = lax.broadcasted_iota(jnp.int32, share.shape, 1)
    width = share.shape[1]
    real = jnp.where(columns < half, ahead, pltpu.roll(behind, half, 1))
    imag = jnp.where(columns < half, pltpu.roll(ahead, width - half, 1), behind)
    out_ref[0:1, :] = real[0:1, :batch]
    out_ref[1:2, :] = imag[0:1, :batch]

    @pl.when(closer)
    def _():
        def done(peer, carry):
            @pl.when(peer != me)
            def _():
                final_copy(peer, place).wait_send()

            return carry

        lax.fori_loop(0, peers, done, 0)

    @pl.when(col < last)
    def _():
        for piece in range(groups * pieces):
            right_copy(piece).wait_send()

    @pl.when(col > 0)
    def _():
        for piece in range(groups * pieces):
            left_copy(piece).wait_send()


def on_device(site_tensors, left_edge, right_edge, order, bitstrings):
    n_col = lax.axis_size("col")
    n_slc = lax.axis_size("slc")
    batch = bitstrings.shape[0]
    half = batch // 2
    groups = GROUPS
    pieces = PIECES
    sites, chi, wide = site_tensors.shape[1], site_tensors.shape[3], site_tensors.shape[4]
    peers = n_col * n_slc
    chunks = groups * pieces
    vmem = pl.BlockSpec(memory_space=pltpu.VMEM)
    smem = pl.BlockSpec(memory_space=pltpu.SMEM)
    hbm = pl.BlockSpec(memory_space=pl.ANY)
    lane_rows = 128
    sizes = [2**size for _, size in segments_of(sites)]
    return pl.pallas_call(
        functools.partial(kernel, n_col, n_slc, groups, pieces),
        out_shape=jax.ShapeDtypeStruct((2, batch), jnp.float32),
        in_specs=[smem, smem, hbm, hbm, hbm],
        out_specs=vmem,
        scratch_shapes=[
            pltpu.VMEM(site_tensors.shape, site_tensors.dtype),
            pltpu.VMEM(left_edge.shape, left_edge.dtype),
            pltpu.VMEM(right_edge.shape, right_edge.dtype),
            pltpu.SemaphoreType.DMA((3,)),
            pltpu.VMEM((len(sizes), max(sizes) // 2 * chi, 2 * wide), jnp.bfloat16),
            pltpu.VMEM((sizes[0], 2 * chi, wide), jnp.bfloat16),
            pltpu.VMEM((sum(sizes[1:]), 2 * chi, 2 * wide), jnp.bfloat16),
            pltpu.VMEM((batch, chi, wide), jnp.float32),
            pltpu.VMEM((batch, chi, wide), jnp.float32),
            pltpu.VMEM((lane_rows, wide), jnp.float32),
            pltpu.VMEM((8, lane_rows), jnp.float32),
            pltpu.VMEM((2 * n_slc, 8, lane_rows), jnp.float32),
            pltpu.SemaphoreType.DMA((chunks,)),
            pltpu.SemaphoreType.DMA((chunks,)),
            pltpu.SemaphoreType.DMA((chunks,)),
            pltpu.SemaphoreType.DMA((chunks,)),
            pltpu.SemaphoreType.DMA((peers,)),
            pltpu.SemaphoreType.DMA((2 * n_slc,)),
        ],
        compiler_params=pltpu.CompilerParams(collective_id=0, has_side_effects=True),
    )(order, bitstrings, site_tensors, left_edge, right_edge)


def solution(mesh):
    return jax.shard_map(
        on_device,
        mesh=mesh,
        in_specs=(
            P(("grp", "slc"), "col", None, None, None),
            P(("grp", "slc"), None, None),
            P(("grp", "slc"), None, None),
            P(("grp", "col")),
            P(("grp", "bat"), None),
        ),
        out_specs=P(None, ("grp", "bat")),
        check_vma=False,
    )
```
